32 devices in a mesh: owner: 8 (over z, y), sub: 4 (over x, core).
Axes of the slice: x: 2, y: 2, z: 4, core: 2. Of those that a mesh axis runs over, the one named last changes fastest.
Arguments:
- velocity: float32 [6, 16384], P(None, 'owner'), may hold values from -6 to 6
- properties: float32 [4, 16384], P(None, 'owner'), may hold values from 0.3 to 3
- first_body: int32 [262144], P(('owner', 'sub')), may hold values from 0 to 16383, as said below
- second_body: int32 [262144], P(('owner', 'sub')), may hold values from 0 to 16383, as said below
- geometry: float32 [9, 262144], P(None, ('owner', 'sub')), may hold values from -2 to 2, as said below
- target_speed: float32 [262144], P(('owner', 'sub')), may hold values from -1 to 2
- warm_impulse: float32 [262144], P(('owner', 'sub')), may hold values from 0 to 0.5
- live_pairs: int32 [2048], P(('owner', 'sub')), may hold values from 0 to 128, as said below
Outputs:
- velocity_out: float32 [6, 16384], P(None, 'owner')
- impulse_out: float32 [262144], P(('owner', 'sub'))
The draws below stay inside these ranges and needn't reach their ends.
Inputs may be any that keep to these rules, and one draw needn't show every extreme that they name: Pair slots are ordered by device of owner+sub, then by partner owner, then by 8 blocks of 128 slots; a slot on a device of owner o with partner owner q has first_body in [o * 2048, (o+1) * 2048) and second_body in [q * 2048, (q+1) * 2048). `second_body`: see first_body. `live_pairs`: on every device the first block toward its own owner is full; live counts differ strongly between devices and between partner owners. `geometry`: rows 0 to 2 of every column have unit length.
All inputs are finite; a program needn't handle non-finite values.
Results may differ from the reference program's by a relative error of at most 0.0001.
Values sent between devices are 32-bit elements; how exact they have to be, the bound alone decides.
A program may use at most 128 MiB of HBM per device.

```python
import math
import jax
import jax.numpy as jnp

B_OWN = 2048
KB = 8
PAIR = 128
ITERS = 4
BODIES = 16384
PAIRS = 262144
BLOCKS = 2048
N_OWNER = 8
N_SUB = 4


def slot_owners():
    slots = jnp.arange(PAIRS, dtype=jnp.int32)
    owner_of = slots // (N_OWNER * KB * PAIR * N_SUB)
    partner = slots // (KB * PAIR) % N_OWNER
    return (owner_of, partner)


def draw_first_body(key, part):
    owner_of, partner = slot_owners()
    return owner_of * B_OWN + jax.random.randint(jax.random.fold_in(key, 11), (PAIRS,), 0, B_OWN, dtype=jnp.int32)


def draw_second_body(key, part):
    owner_of, partner = slot_owners()
    return partner * B_OWN + jax.random.randint(jax.random.fold_in(key, 12), (PAIRS,), 0, B_OWN, dtype=jnp.int32)


def draw_live_pairs(key, part):
    blocks = jnp.arange(BLOCKS, dtype=jnp.int32)
    per_device = N_OWNER * KB
    device = blocks // per_device
    owner_of = device // N_SUB
    partner = blocks // KB % N_OWNER
    apart = jnp.abs(partner - owner_of)
    apart = jnp.minimum(apart, N_OWNER - apart)
    near = (apart <= 1) | (apart == 4)
    level = jax.random.randint(jax.random.fold_in(key, 21), (N_OWNER * N_SUB,), 1, 5, dtype=jnp.int32)[device]
    near_counts = jax.random.randint(jax.random.fold_in(key, 22), (BLOCKS,), PAIR // 2, PAIR + 1, dtype=jnp.int32)
    far_counts = jax.random.randint(jax.random.fold_in(key, 23), (BLOCKS,), 0, PAIR // 4 + 1, dtype=jnp.int32)
    far_counts = jnp.minimum(far_counts * level // 2, PAIR)
    counts = jnp.where(near, near_counts, far_counts)
    own_first = (partner == owner_of) & (blocks % KB == 0)
    return jnp.where(own_first, PAIR, counts).astype(jnp.int32)


def draw_geometry(key, part):
    angle = jax.random.uniform(jax.random.fold_in(key, 31), (PAIRS,), jnp.float32, -3.14159, 3.14159)
    height = jax.random.uniform(jax.random.fold_in(key, 32), (PAIRS,), jnp.float32, -1.0, 1.0)
    radial = jnp.sqrt(jnp.maximum(1.0 - height * height, 0.0))
    normal = jnp.stack([radial * jnp.cos(angle), radial * jnp.sin(angle), height])
    arms = jax.random.uniform(jax.random.fold_in(key, 33), (6, PAIRS), jnp.float32, -1.0, 1.0)
    return jnp.concatenate([normal, arms]).astype(jnp.float32)


def levels(rng, dims, split, low, high):
    gain, own = 1.0, jax.random.fold_in(rng, 6)
    for dim, parts in split:
        draws = jnp.exp(jax.random.uniform(jax.random.fold_in(own, dim), (parts,), jnp.float32, low / len(split), high / len(split)))
        gain = gain * jnp.repeat(draws, dims[dim] // parts).reshape([-1 if axis == dim else 1 for axis in range(len(dims))])
    return gain


def normal_values(rng, dims, width, most, shards=(), held_as=jnp.bfloat16):
    values = jax.random.normal(rng, dims, jnp.float32) * width
    if len(shards) > 0:
        values = levels(rng, dims, shards, -0.22, 0.18) * values
    return jnp.clip(values, min=-most, max=most).astype(held_as)


def setup_inputs(seed: int = 0) -> dict:
    seeds = jax.random.split(jax.random.key(seed), 9)
    return {
        "velocity": normal_values(seeds[0], (6, BODIES), 1.0, 6.0, ((1, 8),), jnp.float32),
        "properties": jnp.clip(jnp.exp(math.log(3.0) - 2.3025851 * jax.random.uniform(seeds[1], (4, BODIES), jnp.float32) ** levels(seeds[1], (4, BODIES), ((1, 8),), -0.2, 0.2)), 0.3, 3.0),
        "first_body": draw_first_body(jax.random.fold_in(seeds[8], 71), 0),
        "second_body": draw_second_body(jax.random.fold_in(seeds[8], 71), 0),
        "geometry": draw_geometry(jax.random.fold_in(seeds[8], 71), 0),
        "target_speed": jnp.clip(-1.0 + 3.0 * jax.random.uniform(seeds[5], (PAIRS,), jnp.float32) ** levels(seeds[5], (PAIRS,), ((0, 32),), -0.2, 0.2), -1.0, 2.0),
        "warm_impulse": jnp.clip(0.5 * jax.random.uniform(seeds[6], (PAIRS,), jnp.float32) ** levels(seeds[6], (PAIRS,), ((0, 32),), -0.2, 0.2), 0.0, 0.5),
        "live_pairs": draw_live_pairs(jax.random.fold_in(seeds[8], 71), 0),
    }


relax = 0.1


def cross_rows(left, right):
    return jnp.stack([left[1] * right[2] - left[2] * right[1],
                      left[2] * right[0] - left[0] * right[2],
                      left[0] * right[1] - left[1] * right[0]])


def reference(velocity, properties, first_body, second_body, geometry, target_speed, warm_impulse, live_pairs):
    slots = jnp.arange(PAIRS, dtype=jnp.int32)
    live = (slots % PAIR) < jnp.repeat(live_pairs, PAIR, total_repeat_length=PAIRS)
    normal = geometry[0:3]
    arm_first = geometry[3:6]
    arm_second = geometry[6:9]
    cross_first = cross_rows(arm_first, normal)
    cross_second = cross_rows(arm_second, normal)
    props_first = properties[:, first_body]
    props_second = properties[:, second_body]
    mass_sum = props_first[0] + props_second[0] + jnp.sum(cross_first * cross_first * props_first[1:4], 0) + jnp.sum(cross_second * cross_second * props_second[1:4], 0)
    speeds = velocity
    impulse = warm_impulse
    for iteration in range(ITERS):
        vel_first = speeds[:, first_body]
        vel_second = speeds[:, second_body]
        relative = vel_first[0:3] + cross_rows(vel_first[3:6], arm_first) - vel_second[0:3] - cross_rows(vel_second[3:6], arm_second)
        normal_speed = jnp.sum(normal * relative, 0)
        change = relax * (target_speed - normal_speed) / mass_sum
        fresh = jnp.where(live, jnp.maximum(impulse + change, 0.0), impulse)
        applied = fresh - impulse
        impulse = fresh
        delta_first = jnp.concatenate([props_first[0] * applied * normal, props_first[1:4] * (applied * cross_first)])
        delta_second = -jnp.concatenate([props_second[0] * applied * normal, props_second[1:4] * (applied * cross_second)])
        total = jnp.zeros(speeds.shape, jnp.float32).at[:, first_body].add(delta_first).at[:, second_body].add(delta_second)
        speeds = speeds + total
    return speeds, impulse
```

```python
import functools

import jax
import jax.numpy as jnp
from jax import lax
from jax.experimental import pallas as pl
from jax.experimental.pallas import tpu as pltpu
from jax.sharding import PartitionSpec as P

ITERS = 4
LANES = 128
VEL = 6
PROPS = 4
relax = 0.1
MESH = pl.DeviceIdType.MESH


def cross_rows(left, right):
    return [
        left[1] * right[2] - left[2] * right[1],
        left[2] * right[0] - left[0] * right[2],
        left[0] * right[1] - left[1] * right[0],
    ]


def peer(position, shift, devices, subs):
    target = lax.rem(position + shift, devices)
    return target, (lax.div(target, subs), lax.rem(target, subs))


def greet(position, devices, subs):
    barrier = pltpu.get_barrier_semaphore()

    def signal(shift, carry):
        _, where = peer(position, shift, devices, subs)
        pl.semaphore_signal(barrier, inc=1, device_id=where, device_id_type=MESH)
        return carry

    lax.fori_loop(1, devices, signal, 0)
    pl.semaphore_wait(barrier, devices - 1)


def spread(position, devices, subs, source, target_ref, send_sem, recv_sem, step=1):
    def copy(shift, slot):
        _, where = peer(position, shift, devices, subs)
        return pltpu.make_async_remote_copy(
            src_ref=source,
            dst_ref=target_ref.at[slot],
            send_sem=send_sem.at[shift - 1],
            recv_sem=recv_sem.at[shift - 1],
            device_id=where,
            device_id_type=MESH,
        )

    def start(shift, carry):
        copy(shift, position).start()
        return carry

    def finish(shift, carry):
        sender = lax.rem(position - shift + devices, devices)
        copy(shift, sender).wait()
        return carry

    lax.fori_loop(1, devices, start, 0)
    lax.fori_loop(1, devices, finish, 0)


def share_kernel(devices, subs, piece_ref, full_ref, send_sem, recv_sem):
    position = lax.axis_index("owner") * subs + lax.axis_index("sub")
    full_ref[position] = piece_ref[...]
    greet(position, devices, subs)
    spread(position, devices, subs, piece_ref, full_ref, send_sem, recv_sem)


def reduce_share_kernel(
    devices, subs, delta_ref, own_ref, full_ref, piece_ref, held, send_sem, recv_sem, send2, recv2
):
    position = lax.axis_index("owner") * subs + lax.axis_index("sub")
    greet(position, devices, subs)

    def copy(shift):
        target, where = peer(position, shift, devices, subs)
        return pltpu.make_async_remote_copy(
            src_ref=delta_ref.at[target],
            dst_ref=held.at[shift - 1],
            send_sem=send_sem.at[shift - 1],
            recv_sem=recv_sem.at[shift - 1],
            device_id=where,
            device_id_type=MESH,
        )

    def start(shift, carry):
        copy(shift).start()
        return carry

    def take(shift, total):
        copy(shift).wait()
        return total + held[shift - 1]

    lax.fori_loop(1, devices, start, 0)
    total = own_ref[...] + delta_ref[position]
    total = lax.fori_loop(1, devices, take, total)
    piece_ref[...] = total
    full_ref[position] = total
    spread(position, devices, subs, piece_ref, full_ref, send2, recv2)


def comm_params(collective_id):
    return pltpu.CompilerParams(collective_id=collective_id, has_side_effects=True)


def vmem_specs(count):
    return [pl.BlockSpec(memory_space=pltpu.VMEM)] * count


def share(piece, devices, subs):
    return pl.pallas_call(
        functools.partial(share_kernel, devices, subs),
        name="share",
        out_shape=jax.ShapeDtypeStruct((devices,) + piece.shape, jnp.float32),
        in_specs=vmem_specs(1),
        out_specs=vmem_specs(1)[0],
        scratch_shapes=[pltpu.SemaphoreType.DMA((devices - 1,))] * 2,
        compiler_params=comm_params(0),
    )(piece)


def reduce_share(delta, own, devices, subs):
    return pl.pallas_call(
        functools.partial(reduce_share_kernel, devices, subs),
        name="reduce_share",
        out_shape=(
            jax.ShapeDtypeStruct(delta.shape, jnp.float32),
            jax.ShapeDtypeStruct(own.shape, jnp.float32),
        ),
        in_specs=vmem_specs(2),
        out_specs=tuple(vmem_specs(2)),
        scratch_shapes=[pltpu.VMEM((devices - 1,) + own.shape, jnp.float32)]
        + [pltpu.SemaphoreType.DMA((devices - 1,))] * 4,
        compiler_params=comm_params(1),
    )(delta, own)


def low_high(index, height):
    chunk = lax.shift_right_logical(index, 7)
    if height & (height - 1) == 0:
        chunk = chunk & (height - 1)
    else:
        chunk = lax.rem(chunk, jnp.full_like(chunk, height))
    return index & (LANES - 1), chunk


def gather_rows(table_ref, base, subs, first_row, rows, part, low, chunk):
    out = [jnp.zeros(low.shape, jnp.float32) for _ in range(rows)]
    for sub in range(subs):
        for c in range(part):
            hit = chunk == sub * part + c
            for row in range(rows):
                line = table_ref[base + sub, pl.ds((first_row + row) * part + c, 1), :]
                picked = jnp.take_along_axis(
                    jnp.broadcast_to(line, low.shape), low, axis=1, mode="promise_in_bounds"
                )
                out[row] = jnp.where(hit, picked, out[row])
    return out


def prepare_kernel(groups, subs, part, table_ref, first_ref, second_ref, geo_ref, coef_ref):
    owner = lax.axis_index("owner")

    def body(q, carry):
        low1, chunk1 = low_high(first_ref[q], subs * part)
        low2, chunk2 = low_high(second_ref[q], subs * part)
        normal = [geo_ref[k, q] for k in range(3)]
        cross1 = cross_rows([geo_ref[3 + k, q] for k in range(3)], normal)
        cross2 = cross_rows([geo_ref[6 + k, q] for k in range(3)], normal)
        props1 = gather_rows(table_ref, owner * subs, subs, VEL, PROPS, part, low1, chunk1)
        props2 = gather_rows(table_ref, q * subs, subs, VEL, PROPS, part, low2, chunk2)
        mass = props1[0] + props2[0]
        for k in range(3):
            mass += cross1[k] * cross1[k] * props1[1 + k]
            mass += cross2[k] * cross2[k] * props2[1 + k]
        values = [relax / mass] + props1 + props2
        for k, value in enumerate(values):
            coef_ref[q, k] = value
        return carry

    lax.fori_loop(0, groups, body, 0)


def place(deltas, low, chunk, height):
    rows = len(deltas)
    tall = lax.broadcasted_iota(jnp.int32, (height, LANES), 0)
    wide = lax.broadcasted_iota(jnp.int32, (LANES, LANES), 0)
    left, right = [], []
    coarse = [d.astype(jnp.bfloat16).astype(jnp.float32) for d in deltas]
    fine = [d - c for d, c in zip(deltas, coarse)]
    for i in range(low.shape[0]):
        hit = tall == jnp.broadcast_to(chunk[i : i + 1], (height, LANES))
        block = [
            jnp.where(hit, jnp.broadcast_to(x[i : i + 1], (height, LANES)), 0.0)
            for x in coarse + fine
        ]
        left.append(jnp.concatenate(block, axis=0).astype(jnp.bfloat16))
        right.append(
            jnp.where(wide == jnp.broadcast_to(low[i : i + 1], (LANES, LANES)), 1.0, 0.0).astype(
                jnp.bfloat16
            )
        )
    out = lax.dot_general(
        jnp.concatenate(left, axis=1),
        jnp.concatenate(right, axis=1),
        (((1,), (1,)), ((), ())),
        preferred_element_type=jnp.float32,
    )
    return out[: rows * height] + out[rows * height :]


def iterate_kernel(
    groups, subs, part, table_ref, first_ref, second_ref, geo_ref, coef_ref, target_ref, live_ref,
    impulse_ref, impulse_out, delta_ref, own_acc
):
    owner = lax.axis_index("owner")
    height = subs * part
    own_acc[...] = jnp.zeros_like(own_acc)

    def body(q, carry):
        low1, chunk1 = low_high(first_ref[q], height)
        low2, chunk2 = low_high(second_ref[q], height)
        normal = [geo_ref[k, q] for k in range(3)]
        cross1 = cross_rows([geo_ref[3 + k, q] for k in range(3)], normal)
        cross2 = cross_rows([geo_ref[6 + k, q] for k in range(3)], normal)
        vel1 = gather_rows(table_ref, owner * subs, subs, 0, VEL, part, low1, chunk1)
        vel2 = gather_rows(table_ref, q * subs, subs, 0, VEL, part, low2, chunk2)
        speed = jnp.zeros_like(vel1[0])
        for k in range(3):
            speed += normal[k] * (vel1[k] - vel2[k])
            speed += cross1[k] * vel1[3 + k] - cross2[k] * vel2[3 + k]
        impulse = impulse_ref[q]
        step = (target_ref[q] - speed) * coef_ref[q, 0]
        lane = lax.broadcasted_iota(jnp.int32, impulse.shape, 1)
        fresh = jnp.where(lane < live_ref[q], jnp.maximum(impulse + step, 0.0), impulse)
        impulse_out[q] = fresh
        applied = fresh - impulse
        delta1 = [coef_ref[q, 1] * applied * normal[k] for k in range(3)]
        delta1 += [coef_ref[q, 2 + k] * (applied * cross1[k]) for k in range(3)]
        delta2 = [-(coef_ref[q, 5] * applied * normal[k]) for k in range(3)]
        delta2 += [-(coef_ref[q, 6 + k] * (applied * cross2[k])) for k in range(3)]
        own_acc[...] += place(delta1, low1, chunk1, height)
        there = place(delta2, low2, chunk2, height)
        for sub in range(subs):
            for row in range(VEL):
                start = row * height + sub * part
                delta_ref[q * subs + sub, pl.ds(row * part, part), :] = there[start : start + part]
        return carry

    lax.fori_loop(0, groups, body, 0)
    for sub in range(subs):
        for row in range(VEL):
            start = row * height + sub * part
            delta_ref[owner * subs + sub, pl.ds(row * part, part), :] += own_acc[
                start : start + part, :
            ]


def on_device(
    groups, subs, velocity, properties, first_body, second_body, geometry, target_speed,
    warm_impulse, live_pairs
):
    owned = velocity.shape[1]
    devices = groups * subs
    part = owned // (LANES * subs)
    count = first_body.shape[0]
    rows = count // (groups * LANES)
    block = count // live_pairs.shape[0]
    tiles = (groups, rows, LANES)
    sub = lax.axis_index("sub")

    def own_piece(array):
        cut = lax.dynamic_slice_in_dim(array, sub * (part * LANES), part * LANES, 1)
        return cut.reshape(-1, LANES)

    own = own_piece(velocity)
    table = share(jnp.concatenate([own, own_piece(properties)], axis=0), devices, subs)
    first = first_body.reshape(tiles)
    second = second_body.reshape(tiles)
    geo = geometry.reshape((geometry.shape[0],) + tiles)
    target = target_speed.reshape(tiles)
    impulse = warm_impulse.reshape(tiles)
    slot = jnp.arange(LANES, dtype=jnp.int32)
    rows_per_block = block // LANES
    offset = jnp.arange(count // LANES, dtype=jnp.int32) % rows_per_block * LANES
    bound = jnp.repeat(live_pairs, rows_per_block, total_repeat_length=count // LANES) - offset
    live = jnp.broadcast_to(bound[:, None], (count // LANES, LANES)).reshape(tiles)

    coef = pl.pallas_call(
        functools.partial(prepare_kernel, groups, subs, part),
        name="prepare",
        out_shape=jax.ShapeDtypeStruct((groups, 9, rows, LANES), jnp.float32),
        in_specs=vmem_specs(4),
        out_specs=vmem_specs(1)[0],
    )(table, first, second, geo)

    step = pl.pallas_call(
        functools.partial(iterate_kernel, groups, subs, part),
        name="iterate",
        out_shape=(
            jax.ShapeDtypeStruct(tiles, jnp.float32),
            jax.ShapeDtypeStruct((devices, VEL * part, LANES), jnp.float32),
        ),
        in_specs=vmem_specs(8),
        out_specs=tuple(vmem_specs(2)),
        scratch_shapes=[pltpu.VMEM((VEL * subs * part, LANES), jnp.float32)],
    )
    for _ in range(ITERS):
        impulse, delta = step(table, first, second, geo, coef, target, live, impulse)
        table, own = reduce_share(delta, own, devices, subs)
    start = lax.axis_index("owner") * subs
    mine = lax.dynamic_slice_in_dim(table, start, subs, 0).reshape(subs, VEL, part, LANES)
    speeds = mine.transpose(1, 0, 2, 3).reshape(VEL, owned)
    return (speeds, impulse.reshape(count))


def solution(mesh):
    groups, subs = mesh.shape["owner"], mesh.shape["sub"]
    return jax.shard_map(
        functools.partial(on_device, groups, subs),
        mesh=mesh,
        in_specs=(
            P(None, "owner"),
            P(None, "owner"),
            P(("owner", "sub")),
            P(("owner", "sub")),
            P(None, ("owner", "sub")),
            P(("owner", "sub")),
            P(("owner", "sub")),
            P(("owner", "sub")),
        ),
        out_specs=(P(None, "owner"), P(("owner", "sub"))),
        check_vma=False,
    )
```

```python
import functools

import jax
import jax.numpy as jnp
from jax import lax
from jax.experimental import pallas as pl
from jax.experimental.pallas import tpu as pltpu
from jax.sharding import PartitionSpec as P

ITERS = 4
LANES = 128
VEL = 6
PROPS = 4
relax = 0.1
MESH = pl.DeviceIdType.MESH


def cross_rows(left, right):
    return [
        left[1] * right[2] - left[2] * right[1],
        left[2] * right[0] - left[0] * right[2],
        left[0] * right[1] - left[1] * right[0],
    ]


def around(index, shift, size):
    return lax.rem(index + shift + size, size)


def greet(groups, subs, owner, sub):
    barrier = pltpu.get_barrier_semaphore()

    def signal(shift, carry):
        where = (around(owner, shift, groups), sub)
        pl.semaphore_signal(barrier, inc=1, device_id=where, device_id_type=MESH)
        return carry

    lax.fori_loop(1, groups, signal, 0)
    for j in range(1, subs):
        where = (owner, around(sub, j, subs))
        pl.semaphore_signal(barrier, inc=1, device_id=where, device_id_type=MESH)
    pl.semaphore_wait(barrier, groups + subs - 2)


def remote(source, target, send_sem, recv_sem, where):
    return pltpu.make_async_remote_copy(
        src_ref=source,
        dst_ref=target,
        send_sem=send_sem,
        recv_sem=recv_sem,
        device_id=where,
        device_id_type=MESH,
    )


def gather_all(groups, subs, owner, sub, piece_ref, full_ref, send3, recv3, send4, recv4):
    def across(k, slot):
        where = (around(owner, k, groups), sub)
        return remote(piece_ref, full_ref.at[slot], send3.at[k - 1], recv3.at[k - 1], where)

    def along(j, k, source, slot):
        where = (owner, around(sub, j, subs))
        return remote(source, full_ref.at[slot], send4.at[j - 1, k], recv4.at[j - 1, k], where)

    def start(k, carry):
        across(k, owner * subs + sub).start()
        return carry

    def relay(k, carry):
        slot = around(owner, -k, groups) * subs + sub
        across(k, slot).wait_recv()
        for j in range(1, subs):
            along(j, k, full_ref.at[slot], slot).start()
        return carry

    def finish(k, carry):
        for j in range(1, subs):
            slot = around(owner, -k, groups) * subs + around(sub, -j, subs)
            along(j, k, piece_ref, slot).wait()
        return carry

    def sent(k, carry):
        across(k, owner * subs + sub).wait_send()
        return carry

    lax.fori_loop(1, groups, start, 0)
    for j in range(1, subs):
        along(j, 0, piece_ref, owner * subs + sub).start()
    lax.fori_loop(1, groups, relay, 0)
    lax.fori_loop(0, groups, finish, 0)
    lax.fori_loop(1, groups, sent, 0)


def share_kernel(groups, subs, piece_ref, full_ref, send3, recv3, send4, recv4):
    owner, sub = lax.axis_index("owner"), lax.axis_index("sub")
    full_ref[owner * subs + sub] = piece_ref[...]
    greet(groups, subs, owner, sub)
    gather_all(groups, subs, owner, sub, piece_ref, full_ref, send3, recv3, send4, recv4)


def reduce_share_kernel(
    groups, subs, last, delta_ref, own_ref, full_ref, piece_ref, held1, held2, reduced,
    send1, recv1, send2, recv2, send3, recv3, send4, recv4
):
    owner, sub = lax.axis_index("owner"), lax.axis_index("sub")
    greet(groups, subs, owner, sub)

    def inner(k, j):
        q, there = around(owner, k, groups), around(sub, j, subs)
        return remote(
            delta_ref.at[q * subs + there],
            held1.at[j - 1, k],
            send1.at[j - 1, k],
            recv1.at[j - 1, k],
            (owner, there),
        )

    def outer(k):
        where = (around(owner, k, groups), sub)
        return remote(
            reduced.at[k - 1], held2.at[k - 1], send2.at[k - 1], recv2.at[k - 1], where
        )

    def start(k, carry):
        for j in range(1, subs):
            inner(k, j).start()
        return carry

    def summed(k):
        total = delta_ref[around(owner, k, groups) * subs + sub]
        for j in range(1, subs):
            inner(k, j).wait_recv()
            total += held1[j - 1, k]
        return total

    def pass_on(k, carry):
        reduced[k - 1] = summed(k)
        outer(k).start()
        return carry

    def take(k, total):
        outer(k).wait()
        return total + held2[k - 1]

    def sent(k, carry):
        for j in range(1, subs):
            inner(k, j).wait_send()
        return carry

    lax.fori_loop(1, groups, start, 0)
    start(0, 0)
    lax.fori_loop(1, groups, pass_on, 0)
    total = own_ref[...] + summed(0)
    total = lax.fori_loop(1, groups, take, total)
    lax.fori_loop(0, groups, sent, 0)
    piece_ref[...] = total
    if last:
        full_ref[sub] = total

        def along(j, slot):
            where = (owner, around(sub, j, subs))
            return remote(
                piece_ref, full_ref.at[slot], send4.at[j - 1, 0], recv4.at[j - 1, 0], where
            )

        for j in range(1, subs):
            along(j, sub).start()
        for j in range(1, subs):
            along(j, around(sub, -j, subs)).wait()
    else:
        full_ref[owner * subs + sub] = total
        gather_all(groups, subs, owner, sub, piece_ref, full_ref, send3, recv3, send4, recv4)


def comm_params(collective_id):
    return pltpu.CompilerParams(collective_id=collective_id, has_side_effects=True)


def vmem_specs(count):
    return [pl.BlockSpec(memory_space=pltpu.VMEM)] * count


def semaphores(groups, subs, wide):
    shape = (subs - 1, groups) if wide else (groups - 1,)
    return [pltpu.SemaphoreType.DMA(shape)] * 2


def share(piece, groups, subs):
    return pl.pallas_call(
        functools.partial(share_kernel, groups, subs),
        name="share",
        out_shape=jax.ShapeDtypeStruct((groups * subs,) + piece.shape, jnp.float32),
        in_specs=vmem_specs(1),
        out_specs=vmem_specs(1)[0],
        scratch_shapes=semaphores(groups, subs, False) + semaphores(groups, subs, True),
        compiler_params=comm_params(0),
    )(piece)


def reduce_share(delta, own, groups, subs, last):
    pieces = subs if last else groups * subs
    return pl.pallas_call(
        functools.partial(reduce_share_kernel, groups, subs, last),
        name="reduce_last" if last else "reduce_share",
        out_shape=(
            jax.ShapeDtypeStruct((pieces,) + own.shape, jnp.float32),
            jax.ShapeDtypeStruct(own.shape, jnp.float32),
        ),
        in_specs=vmem_specs(2),
        out_specs=tuple(vmem_specs(2)),
        scratch_shapes=[
            pltpu.VMEM((subs - 1, groups) + own.shape, jnp.float32),
            pltpu.VMEM((groups - 1,) + own.shape, jnp.float32),
            pltpu.VMEM((groups - 1,) + own.shape, jnp.float32),
        ]
        + semaphores(groups, subs, True)
        + semaphores(groups, subs, False) * 2
        + semaphores(groups, subs, True),
        compiler_params=comm_params(2 if last else 1),
    )(delta, own)


def low_high(index, height):
    chunk = lax.shift_right_logical(index, 7)
    if height & (height - 1) == 0:
        chunk = chunk & (height - 1)
    else:
        chunk = lax.rem(chunk, jnp.full_like(chunk, height))
    return index & (LANES - 1), chunk


def gather_rows(table_ref, base, subs, first_row, rows, part, low, chunk):
    out = [jnp.zeros(low.shape, jnp.float32) for _ in range(rows)]
    for sub in range(subs):
        for c in range(part):
            hit = chunk == sub * part + c
            for row in range(rows):
                line = table_ref[base + sub, pl.ds((first_row + row) * part + c, 1), :]
                picked = jnp.take_along_axis(
                    jnp.broadcast_to(line, low.shape), low, axis=1, mode="promise_in_bounds"
                )
                out[row] = jnp.where(hit, picked, out[row])
    return out


def prepare_kernel(groups, subs, part, table_ref, first_ref, second_ref, geo_ref, coef_ref):
    owner = lax.axis_index("owner")

    def body(q, carry):
        low1, chunk1 = low_high(first_ref[q], subs * part)
        low2, chunk2 = low_high(second_ref[q], subs * part)
        normal = [geo_ref[k, q] for k in range(3)]
        cross1 = cross_rows([geo_ref[3 + k, q] for k in range(3)], normal)
        cross2 = cross_rows([geo_ref[6 + k, q] for k in range(3)], normal)
        props1 = gather_rows(table_ref, owner * subs, subs, VEL, PROPS, part, low1, chunk1)
        props2 = gather_rows(table_ref, q * subs, subs, VEL, PROPS, part, low2, chunk2)
        mass = props1[0] + props2[0]
        for k in range(3):
            mass += cross1[k] * cross1[k] * props1[1 + k]
            mass += cross2[k] * cross2[k] * props2[1 + k]
        values = [relax / mass] + props1 + props2
        for k, value in enumerate(values):
            coef_ref[q, k] = value
        return carry

    lax.fori_loop(0, groups, body, 0)


def place(deltas, low, chunk, height):
    rows = len(deltas)
    tall = lax.broadcasted_iota(jnp.int32, (height, LANES), 0)
    wide = lax.broadcasted_iota(jnp.int32, (LANES, LANES), 0)
    left, right = [], []
    coarse = [d.astype(jnp.bfloat16).astype(jnp.float32) for d in deltas]
    fine = [d - c for d, c in zip(deltas, coarse)]
    for i in range(low.shape[0]):
        hit = tall == jnp.broadcast_to(chunk[i : i + 1], (height, LANES))
        block = [
            jnp.where(hit, jnp.broadcast_to(x[i : i + 1], (height, LANES)), 0.0)
            for x in coarse + fine
        ]
        left.append(jnp.concatenate(block, axis=0).astype(jnp.bfloat16))
        right.append(
            jnp.where(wide == jnp.broadcast_to(low[i : i + 1], (LANES, LANES)), 1.0, 0.0).astype(
                jnp.bfloat16
            )
        )
    out = lax.dot_general(
        jnp.concatenate(left, axis=1),
        jnp.concatenate(right, axis=1),
        (((1,), (1,)), ((), ())),
        preferred_element_type=jnp.float32,
    )
    return out[: rows * height] + out[rows * height :]


def iterate_kernel(
    groups, subs, part, table_ref, first_ref, second_ref, geo_ref, coef_ref, target_ref, live_ref,
    impulse_ref, impulse_out, delta_ref, own_acc
):
    owner = lax.axis_index("owner")
    height = subs * part
    own_acc[...] = jnp.zeros_like(own_acc)

    def body(q, carry):
        low1, chunk1 = low_high(first_ref[q], height)
        low2, chunk2 = low_high(second_ref[q], height)
        normal = [geo_ref[k, q] for k in range(3)]
        cross1 = cross_rows([geo_ref[3 + k, q] for k in range(3)], normal)
        cross2 = cross_rows([geo_ref[6 + k, q] for k in range(3)], normal)
        vel1 = gather_rows(table_ref, owner * subs, subs, 0, VEL, part, low1, chunk1)
        vel2 = gather_rows(table_ref, q * subs, subs, 0, VEL, part, low2, chunk2)
        speed = jnp.zeros_like(vel1[0])
        for k in range(3):
            speed += normal[k] * (vel1[k] - vel2[k])
            speed += cross1[k] * vel1[3 + k] - cross2[k] * vel2[3 + k]
        impulse = impulse_ref[q]
        step = (target_ref[q] - speed) * coef_ref[q, 0]
        lane = lax.broadcasted_iota(jnp.int32, impulse.shape, 1)
        fresh = jnp.where(lane < live_ref[q], jnp.maximum(impulse + step, 0.0), impulse)
        impulse_out[q] = fresh
        applied = fresh - impulse
        delta1 = [coef_ref[q, 1] * applied * normal[k] for k in range(3)]
        delta1 += [coef_ref[q, 2 + k] * (applied * cross1[k]) for k in range(3)]
        delta2 = [-(coef_ref[q, 5] * applied * normal[k]) for k in range(3)]
        delta2 += [-(coef_ref[q, 6 + k] * (applied * cross2[k])) for k in range(3)]
        own_acc[...] += place(delta1, low1, chunk1, height)
        there = place(delta2, low2, chunk2, height)
        for sub in range(subs):
            for row in range(VEL):
                start = row * height + sub * part
                delta_ref[q * subs + sub, pl.ds(row * part, part), :] = there[start : start + part]
        return carry

    lax.fori_loop(0, groups, body, 0)
    for sub in range(subs):
        for row in range(VEL):
            start = row * height + sub * part
            delta_ref[owner * subs + sub, pl.ds(row * part, part), :] += own_acc[
                start : start + part, :
            ]


def on_device(
    groups, subs, velocity, properties, first_body, second_body, geometry, target_speed,
    warm_impulse, live_pairs
):
    owned = velocity.shape[1]
    devices = groups * subs
    part = owned // (LANES * subs)
    count = first_body.shape[0]
    rows = count // (groups * LANES)
    block = count // live_pairs.shape[0]
    tiles = (groups, rows, LANES)
    sub = lax.axis_index("sub")

    def own_piece(array):
        cut = lax.dynamic_slice_in_dim(array, sub * (part * LANES), part * LANES, 1)
        return cut.reshape(-1, LANES)

    own = own_piece(velocity)
    table = share(jnp.concatenate([own, own_piece(properties)], axis=0), groups, subs)
    first = first_body.reshape(tiles)
    second = second_body.reshape(tiles)
    geo = geometry.reshape((geometry.shape[0],) + tiles)
    target = target_speed.reshape(tiles)
    impulse = warm_impulse.reshape(tiles)
    slot = jnp.arange(LANES, dtype=jnp.int32)
    rows_per_block = block // LANES
    offset = jnp.arange(count // LANES, dtype=jnp.int32) % rows_per_block * LANES
    bound = jnp.repeat(live_pairs, rows_per_block, total_repeat_length=count // LANES) - offset
    live = jnp.broadcast_to(bound[:, None], (count // LANES, LANES)).reshape(tiles)

    coef = pl.pallas_call(
        functools.partial(prepare_kernel, groups, subs, part),
        name="prepare",
        out_shape=jax.ShapeDtypeStruct((groups, 9, rows, LANES), jnp.float32),
        in_specs=vmem_specs(4),
        out_specs=vmem_specs(1)[0],
    )(table, first, second, geo)

    step = pl.pallas_call(
        functools.partial(iterate_kernel, groups, subs, part),
        name="iterate",
        out_shape=(
            jax.ShapeDtypeStruct(tiles, jnp.float32),
            jax.ShapeDtypeStruct((devices, VEL * part, LANES), jnp.float32),
        ),
        in_specs=vmem_specs(8),
        out_specs=tuple(vmem_specs(2)),
        scratch_shapes=[pltpu.VMEM((VEL * subs * part, LANES), jnp.float32)],
    )
    for iteration in range(ITERS):
        impulse, delta = step(table, first, second, geo, coef, target, live, impulse)
        table, own = reduce_share(delta, own, groups, subs, iteration == ITERS - 1)
    mine = table.reshape(subs, VEL, part, LANES)
    speeds = mine.transpose(1, 0, 2, 3).reshape(VEL, owned)
    return (speeds, impulse.reshape(count))


def solution(mesh):
    groups, subs = mesh.shape["owner"], mesh.shape["sub"]
    return jax.shard_map(
        functools.partial(on_device, groups, subs),
        mesh=mesh,
        in_specs=(
            P(None, "owner"),
            P(None, "owner"),
            P(("owner", "sub")),
            P(("owner", "sub")),
            P(None, ("owner", "sub")),
            P(("owner", "sub")),
            P(("owner", "sub")),
            P(("owner", "sub")),
        ),
        out_specs=(P(None, "owner"), P(("owner", "sub"))),
        check_vma=False,
    )
```
